32 devices in a mesh: state: 8 (over y, x, core), horizon: 4 (over z).
Axes of the slice: x: 2, y: 2, z: 4, core: 2. Of those that a mesh axis runs over, the one named last changes fastest.
Arguments:
- expect: bfloat16 [512, 262144], P('horizon', 'state'), may hold values from -0.00048828125 to 0.00048828125
- steady_dist: float32 [262144], P('state'), may hold values from 0.2 to 2
- policy_deriv: bfloat16 [128, 262144], P('horizon', 'state'), may hold values from -6 to 6
- lottery_index: int32 [128, 2048], P('state'), may hold values from 0 to 2046, as said below
- type_trans: float32 [16, 16], replicated, may hold values from 0.1 to 1
- migration: bfloat16 [8, 2, 16], P('state'), may hold values from 0.049804688 to 0.29882812
- discount: float32 [512], P('horizon'), may hold values from 0.3 to 1
Outputs:
- jacobian: float32 [128, 512], P('state', 'horizon')
- present_value: float32 [128, 512], P('state', 'horizon')
The draws below stay inside these ranges and needn't reach their ends.
Inputs may be any that keep to these rules, and one draw needn't show every extreme that they name: `lottery_index`: for every row and every block of 128 asset nodes, every index of the block lies between 128 * (m // 128) and 128 * (m // 128) + 254, where m is the block's smallest index.
All inputs are finite; a program needn't handle non-finite values.
Results may differ from the reference program's by a relative error of at most 0.0072.
Values may be sent and summed in bfloat16 or wider, within the bound.
No kernel may reach another device: no remote copies, remote signals or barrier semaphores. Data moves between devices by JAX's collectives and lax.ppermute only.
A program may use at most 128 MiB of HBM per device.

```python
import math
import jax
import jax.numpy as jnp
from jax import lax

ASSETS = 2048
COLS = 128
TYPES = 16
STATES_DEV = 32768
REGIONS = 8
RESPONSE_PERIODS = 512
N_STATE = 8


def draw_lottery_index(key, part):
    base_key = jax.random.fold_in(key, 11)
    band_key, node_random_key = jax.random.split(base_key)
    blocks = ASSETS // 128
    row_count = REGIONS * TYPES
    block_ids = jnp.arange(blocks, dtype=jnp.int32)[None, :]
    starts = jnp.clip(block_ids + jax.random.randint(band_key, (row_count, blocks), -1, 1), 0, blocks - 2)
    offsets = jax.random.randint(node_random_key, (row_count, blocks, 128), 0, 255)
    offsets = offsets.at[:, :, 0].set(0).at[:, :, 1].set(254)
    return (128 * starts[:, :, None] + offsets).reshape(row_count, ASSETS).astype(jnp.int32)


def draw_discount(key, part):
    base_key = jax.random.fold_in(key, 23)
    rate_key, where_key, size_key = jax.random.split(base_key, 3)
    switching_intensities = jax.random.uniform(rate_key, (RESPONSE_PERIODS,), minval=0.0, maxval=2.0 / RESPONSE_PERIODS)
    wealth_points = jax.random.randint(where_key, (3,), 0, RESPONSE_PERIODS)
    patience_betas = jax.random.uniform(size_key, (3,), minval=0.5, maxval=0.8)
    impulse_pulses = jnp.ones((RESPONSE_PERIODS,), jnp.float32).at[wealth_points].multiply(patience_betas)
    return (jnp.exp(-switching_intensities) * impulse_pulses).astype(jnp.float32)


def raised(entries, own_key, source, target, parts, factor):
    def block_of(position):
        return (jnp.arange(entries.shape[position]) // (entries.shape[position] // parts)).reshape((-1,) + (1,) * (entries.ndim - 1 - position))

    first = jax.random.permutation(own_key, parts)[block_of(target)]
    other_side = (block_of(target) + parts // 2) % parts
    return jnp.where((block_of(source) == first) | (block_of(source) == other_side), factor * entries, entries)


def steps_of(own_key, shape, cuts, least, high):
    def one(axis_at, parts):
        heights = jax.random.uniform(jax.random.fold_in(jax.random.fold_in(own_key, 6), axis_at), (parts,), jnp.float32, least / len(cuts), high / len(cuts))
        return jnp.repeat(jnp.exp(heights), shape[axis_at] // parts).reshape((-1,) + (1,) * (len(shape) - axis_at - 1))

    level = one(*cuts[0])
    for cut in cuts[1:]:
        level = level * one(*cut)
    return level


def noise(key, dims, scale, reach, shards=(), held_as=jnp.bfloat16):
    factor_of = steps_of(key, dims, shards, -0.22, 0.18) if shards else 1.0
    drawn = jax.random.normal(key, dims, jnp.float32) * scale * factor_of
    return jnp.minimum(jnp.maximum(drawn, -reach), reach).astype(held_as)


def bell_draw_with(rng, dims, deviation, limit, pieces, heavy, kind=jnp.bfloat16):
    values = deviation * jax.random.normal(rng, dims, jnp.float32)
    if pieces:
        values = values * steps_of(rng, dims, pieces, -0.22, 0.18)
    return jnp.clip(raised(values, jax.random.fold_in(rng, 3), *heavy), -limit, limit).astype(kind)


def setup_inputs(seed: int = 0) -> dict:
    key_of = jax.random.split(jax.random.key(seed), 8)
    expect = noise(key_of[0], (RESPONSE_PERIODS, REGIONS * STATES_DEV), (512 * STATES_DEV * N_STATE) ** -0.5, 0.00048828125, ((0, 4), (1, 8)))
    steady_dist = jnp.clip(jnp.exp(math.log(2.0) - 2.3025851 * jax.random.uniform(key_of[1], (REGIONS * STATES_DEV,), jnp.float32) ** steps_of(key_of[1], (REGIONS * STATES_DEV,), ((0, 8),), -0.2, 0.2)), 0.2, 2.0)
    policy_deriv = bell_draw_with(key_of[2], (COLS, REGIONS * STATES_DEV), 1.0, 6.0, ((0, 4), (1, 8)), (1, 0, 8, 2.0))
    lottery_index = draw_lottery_index(jax.random.fold_in(key_of[7], 71), 0)
    type_trans = jnp.clip(jnp.exp(jax.random.uniform(key_of[4], (TYPES, TYPES), jnp.float32, math.log(0.1), math.log(1.0))), 0.1, 1.0)
    migration = jnp.clip(0.049804688 + 0.24902344 * jax.random.uniform(key_of[5], (REGIONS, 2, TYPES), jnp.float32) ** steps_of(key_of[5], (REGIONS, 2, TYPES), ((0, 8),), -0.2, 0.2), 0.049804688, 0.29882812).astype(jnp.bfloat16)
    discount = draw_discount(jax.random.fold_in(key_of[7], 71), 0)
    return dict(expect=expect, steady_dist=steady_dist, policy_deriv=policy_deriv, lottery_index=lottery_index, type_trans=type_trans, migration=migration, discount=discount)


def region_shift(policy_cols, steady_cols, lottery_rows, type_mix):
    num_cols = policy_cols.shape[0]
    household_type_count = lottery_rows.shape[0]
    num_assets = lottery_rows.shape[1]
    rounded = (steady_cols[None, :] * policy_cols.astype(jnp.float32)).astype(jnp.bfloat16)
    rounded = lax.optimization_barrier(rounded)
    weights = rounded.astype(jnp.float32).reshape(num_cols, household_type_count, num_assets)
    type_rows = lax.broadcasted_iota(jnp.int32, (household_type_count, num_assets), 0)
    landed = jnp.zeros((num_cols, household_type_count, num_assets), jnp.float32)
    landed = landed.at[:, type_rows, lottery_rows].add(weights)
    landed = landed.at[:, type_rows, lottery_rows + 1].add(-weights)
    blended = jnp.einsum("cxa,xy->cya", landed, type_mix, precision=lax.Precision.HIGHEST)
    return blended.reshape(num_cols, household_type_count * num_assets).astype(jnp.bfloat16)


def weigh(entering_lines, switching_intensities):
    height = entering_lines.shape[0]
    scaled = entering_lines.astype(jnp.float32).reshape(height, switching_intensities.shape[0], -1) * switching_intensities[None, :, None]
    return scaled.reshape(height, -1).astype(jnp.bfloat16)


def reference(expect, steady_dist, policy_deriv, lottery_index, type_trans, migration, discount):
    regions = migration.shape[0]
    horizons = expect.shape[0]
    type_mix = type_trans / jnp.sum(type_trans, axis=1, keepdims=True)
    all_rates = migration.astype(jnp.float32)

    def one_region(flow_sum, region):
        start = (region * STATES_DEV).astype(jnp.int32)
        shift_cols = region_shift(
            lax.dynamic_slice_in_dim(policy_deriv, start, STATES_DEV, 1),
            lax.dynamic_slice_in_dim(steady_dist, start, STATES_DEV, 0),
            lax.dynamic_slice_in_dim(lottery_index, (region * TYPES).astype(jnp.int32), TYPES, 0),
            type_mix)
        higher_begin = (((region + 1) % regions) * STATES_DEV).astype(jnp.int32)
        lower_start = (((region + regions - 1) % regions) * STATES_DEV).astype(jnp.int32)
        region_rates = lax.dynamic_index_in_dim(all_rates, region.astype(jnp.int32), 0, keepdims=False)
        stay_rates = 1.0 - region_rates[0] - region_rates[1]
        weighted = (
            weigh(lax.dynamic_slice_in_dim(expect, start, STATES_DEV, 1), stay_rates),
            weigh(lax.dynamic_slice_in_dim(expect, higher_begin, STATES_DEV, 1), region_rates[1]),
            weigh(lax.dynamic_slice_in_dim(expect, lower_start, STATES_DEV, 1), region_rates[0]),
        )
        for part_rows in weighted:
            flow_sum = flow_sum + jnp.dot(shift_cols, part_rows.T, preferred_element_type=jnp.float32)
        return flow_sum, None

    flow_total, _ = lax.scan(one_region, jnp.zeros((COLS, horizons), jnp.float32),
                             jnp.arange(regions, dtype=jnp.int32))

    def diagonal_row(previous, row_now):
        shifted = jnp.concatenate([jnp.zeros((1,), jnp.float32), previous[:-1]])
        current = row_now + shifted
        return current, current

    _, jacobian = lax.scan(diagonal_row, jnp.zeros((horizons,), jnp.float32), flow_total)

    def backward(carried_over, item):
        column_now, factor = item
        current = column_now + factor * carried_over
        return current, current

    _, values = lax.scan(backward, jnp.zeros((COLS,), jnp.float32), (jacobian.T, discount), reverse=True)
    return jacobian, values.T
```

```python
import functools

import jax
import jax.numpy as jnp
from jax import lax
from jax.experimental import pallas as pl
from jax.experimental.pallas import tpu as pltpu
from jax.sharding import PartitionSpec as P

LANES = 128
GROUP = 16


def type_chunks(types):
    first = max(types // 8, 1)
    mid = types // 4
    helped = [first, mid]
    rest = types - 2 * first - 2 * mid
    return [first, mid, rest], helped


def shift_kernel(types, blocks, counts, starts, policy, steady, index, mix_rows, extra, *refs):
    outs, landed = refs[:-1], refs[-1]
    assets = blocks * LANES
    groups = policy.shape[0] // GROUP
    x = pl.program_id(0)

    landed[:, x] = jnp.zeros(landed.shape[:1] + landed.shape[2:], jnp.float32)
    targets = lax.broadcasted_iota(jnp.int32, (2 * LANES, LANES), 0).astype(jnp.float32).astype(jnp.bfloat16)
    one = jnp.ones((2 * LANES, LANES), jnp.bfloat16)
    zero = jnp.zeros((2 * LANES, LANES), jnp.bfloat16)
    for k in range(blocks):
        cut = slice(k * LANES, (k + 1) * LANES)
        begin = starts[x, k] * LANES
        offset = (index[k:k + 1, :] - begin).astype(jnp.float32)
        low = offset.astype(jnp.bfloat16)
        high = (offset + 1.0).astype(jnp.bfloat16)
        lottery = jnp.where(targets == low, one, jnp.where(targets == high, -one, zero))
        weight = steady[k:k + 1, :]
        mass = (weight * policy[:, cut].astype(jnp.float32)).astype(jnp.bfloat16)
        moved = lax.dot_general(mass, lottery, (((1,), (1,)), ((), ())), preferred_element_type=jnp.float32)
        window = pl.ds(pl.multiple_of(begin, LANES), 2 * LANES)
        for g in range(groups):
            landed[g, x, :, window] += moved[g * GROUP:(g + 1) * GROUP]

    @pl.when(x == types - 1)
    def _():
        size = types * GROUP
        row = lax.broadcasted_iota(jnp.int32, (size, size), 0) % GROUP
        col = lax.broadcasted_iota(jnp.int32, (size, size), 1) % GROUP
        spread = jnp.concatenate(
            [jnp.broadcast_to(mix_rows[y:y + 1, :], (GROUP, size)) for y in range(types)], axis=0)
        spread = jnp.where(row == col, spread, 0.0)
        mix_hi = spread.astype(jnp.bfloat16)
        mix_lo = (spread - mix_hi.astype(jnp.float32)).astype(jnp.bfloat16)
        wide = 2 * LANES

        def tile(j, peaks):
            lanes = pl.ds(pl.multiple_of(j * wide, wide), wide)
            peaks = list(peaks)
            for g in range(groups):
                value = landed[g, :, :, lanes].reshape(size, wide)
                hi = value.astype(jnp.bfloat16)
                lo = (value - hi.astype(jnp.float32)).astype(jnp.bfloat16)
                dot = functools.partial(jnp.dot, preferred_element_type=jnp.float32)
                blended = dot(mix_hi, hi) + dot(mix_hi, lo) + dot(mix_lo, hi)
                y = 0
                for c, count in enumerate(counts):
                    for i in range(count):
                        outs[c][g * GROUP:(g + 1) * GROUP,
                                pl.ds(pl.multiple_of(i * assets + j * wide, wide), wide)] = (
                            blended[y * GROUP:(y + 1) * GROUP].astype(jnp.bfloat16))
                        peaks[g] = jnp.maximum(peaks[g], jnp.abs(blended[y * GROUP:(y + 1) * GROUP]))
                        y += 1
            return tuple(peaks)

        peaks = lax.fori_loop(0, assets // wide, tile, (jnp.zeros((GROUP, wide), jnp.float32),) * groups)
        peak = jnp.concatenate([jnp.max(p, axis=1, keepdims=True) for p in peaks], axis=0)
        lane = lax.broadcasted_iota(jnp.int32, extra.shape, 1)
        outs[0][:, counts[0] * assets:] = jnp.where(
            lane < LANES // 2, extra[...].astype(jnp.float32), peak).astype(jnp.bfloat16)


def build_shift(policy, steady, index, type_trans, extra, counts):
    cols = policy.shape[0]
    types, assets = index.shape
    blocks = assets // LANES
    index = index.reshape(types * blocks, LANES)
    starts = (jnp.min(index, axis=1) // LANES).reshape(types, blocks)
    mix = type_trans / jnp.sum(type_trans, axis=1, keepdims=True)
    mix_rows = jnp.repeat(mix.T, GROUP, axis=1)
    shapes = [jax.ShapeDtypeStruct((cols, n * assets + (0 if c else LANES)), jnp.bfloat16)
              for c, n in enumerate(counts)]
    whole = lambda shape: pl.BlockSpec(shape, lambda x, *_: (0,) * len(shape))
    return pl.pallas_call(
        functools.partial(shift_kernel, types, blocks, tuple(counts)),
        out_shape=shapes,
        grid_spec=pltpu.PrefetchScalarGridSpec(
            num_scalar_prefetch=1,
            grid=(types,),
            in_specs=[
                pl.BlockSpec((cols, assets), lambda x, *_: (0, x)),
                pl.BlockSpec((blocks, LANES), lambda x, *_: (x, 0)),
                pl.BlockSpec((blocks, LANES), lambda x, *_: (x, 0)),
                whole((types, types * GROUP)),
                whole((cols, LANES)),
            ],
            out_specs=[whole(s.shape) for s in shapes],
            scratch_shapes=[pltpu.VMEM((cols // GROUP, types, GROUP, assets + LANES), jnp.float32)],
        ),
        compiler_params=pltpu.CompilerParams(
            dimension_semantics=("arbitrary",), vmem_limit_bytes=24 * 2**20),
        cost_estimate=pl.CostEstimate(flops=10**10, bytes_accessed=2**23, transcendentals=0),
        name="build_shift",
    )(starts, policy, steady.reshape(types * blocks, LANES), index, mix_rows, extra)


def product_kernel(n_left, n_right, at, stay, *refs):
    lefts, rights = refs[:n_left], refs[n_left:n_left + n_right]
    out = refs[-1]
    step = pl.program_id(0)

    @pl.when(step == 0)
    def _():
        out[...] = jnp.zeros_like(out)

    scale = stay[0, at + step]
    undo = stay[1, at + step]
    left = jnp.concatenate([r[...] for r in lefts], axis=0)
    sides = []
    for r in rights:
        exact = r[...]
        value = exact.astype(jnp.float32)
        home = (value * scale).astype(jnp.bfloat16).astype(jnp.float32)
        sides += [exact, (home * undo - value).astype(jnp.bfloat16)]
    right = jnp.concatenate(sides, axis=0)
    total = lax.dot_general(left, right, (((1,), (1,)), ((), ())), preferred_element_type=jnp.float32)
    half, width = total.shape[0] // 2, rights[0].shape[0]
    both = total[:half] + total[half:]
    for i in range(n_right):
        base = 2 * i * width
        out[:, i * width:(i + 1) * width] += both[:, base:base + width] + both[:, base + width:base + 2 * width]


def product(lefts, rights, stay, left_at, right_at, count, assets):
    rows = sum(l.shape[0] for l in lefts)
    cols = sum(r.shape[0] for r in rights)
    where = lambda o: lambda i, *_: (0, o + i)
    specs = [pl.BlockSpec((l.shape[0], assets), where(left_at)) for l in lefts]
    specs += [pl.BlockSpec((r.shape[0], assets), where(o)) for r, o in zip(rights, right_at)]
    return pl.pallas_call(
        functools.partial(product_kernel, len(lefts), len(rights), right_at[0]),
        out_shape=jax.ShapeDtypeStruct((rows // 2, cols), jnp.float32),
        grid_spec=pltpu.PrefetchScalarGridSpec(
            num_scalar_prefetch=1,
            grid=(count,),
            in_specs=specs,
            out_specs=pl.BlockSpec((rows // 2, cols), lambda i, *_: (0, 0)),
        ),
        compiler_params=pltpu.CompilerParams(
            dimension_semantics=("arbitrary",), vmem_limit_bytes=24 * 2**20),
        cost_estimate=pl.CostEstimate(
            flops=4 * rows * cols * count * assets, bytes_accessed=2 * (rows + cols) * count * assets,
            transcendentals=0),
        name="product",
    )(stay, *lefts, *rights)


def halves(value):
    high = lax.reduce_precision(value, 8, 7)
    return high.astype(jnp.bfloat16), (value - high).astype(jnp.bfloat16)


def wide(value):
    return value.astype(jnp.float32)


def diagonal(block):
    rows, width = block.shape
    offset = 1
    while offset < rows:
        block = block + jnp.pad(block, ((offset, 0), (offset, 0)))[:rows, :width]
        offset *= 2
    return block


FINE = 2048.0


def local(expect, steady_dist, policy_deriv, lottery_index, type_trans, migration, discount):
    types, assets = lottery_index.shape
    n_state, n_hor = lax.axis_size("state"), lax.axis_size("horizon")
    me = lax.axis_index("horizon")
    width = expect.shape[0]
    cols = policy_deriv.shape[0]
    line = n_hor == 4
    plain, helped = type_chunks(types)
    if not line:
        plain, helped = plain + helped, []
    counts = plain + ([sum(helped)] if helped else [])
    scope = jax.named_scope

    own = migration[0]
    stay = 1.0 - wide(own[0]) - wide(own[1])
    scales = jnp.stack([stay, 1.0 / stay])
    extra = jnp.pad(own, ((0, cols - 2), (0, LANES - types)))

    up = [(i, (i + 1) % n_state) for i in range(n_state)]
    down = [((i + 1) % n_state, i) for i in range(n_state)]
    inward = [(0, 1), (n_hor - 1, n_hor - 2)]
    outward = [(1, 0), (n_hor - 2, n_hor - 1)]
    middle = [(1, 2), (2, 1)]
    moved, at = [], sum(plain)
    for i, n in enumerate(helped):
        with scope(f"lend{i}"):
            moved.append(lax.ppermute(expect[:, at * assets:(at + n) * assets], "horizon", inward))
        at += n

    with scope("build"):
        shift = build_shift(policy_deriv, steady_dist, lottery_index, type_trans, extra, counts)
    above, below = [], []
    for c, d in enumerate(shift):
        with scope(f"fall{c}"):
            above.append(lax.ppermute(d, "state", down))
        with scope(f"rise{c}"):
            below.append(lax.ppermute(d, "state", up))

    each = lambda rate: jnp.broadcast_to(rate[:, None], (types, assets)).reshape(1, types * assets)
    edge = counts[0] * assets
    stay_lanes = each(stay)
    down_lanes = each(wide(above[0][0, edge:edge + types]))
    up_lanes = each(wide(below[0][1, edge:edge + types]))
    coarse = discount.astype(jnp.float16)
    fine = ((discount - wide(coarse)) * FINE).astype(jnp.float16)
    tail = jnp.pad(jnp.stack([coarse, fine]), ((0, cols - 2), (0, 0)))
    bound = sum(wide(v[0][:, edge + LANES // 2:]) for v in (shift, above, below))
    power = jnp.clip(13.0 - jnp.ceil(jnp.log2(jnp.maximum(bound, 1e-30))), -100.0, 100.0)
    raise_by, lower_by = jnp.exp2(power)[:, :1], []
    tail = jnp.concatenate([tail, jnp.pad(power, ((0, 0), (0, LANES // 2))).astype(jnp.float16)], axis=1)

    pieces = aside = None
    all_discount = None
    at = 0
    for c, n in enumerate(counts):
        lanes = n * assets
        span = slice(at * assets, at * assets + lanes)
        with scope(f"mix{c}"):
            joined = (wide(shift[c][:, :lanes]) * stay_lanes[:, span]
                      + wide(above[c][:, :lanes]) * down_lanes[:, span]
                      + wide(below[c][:, :lanes]) * up_lanes[:, span])
            g = (joined * raise_by).astype(jnp.float16)
            if c == 0:
                g = jnp.concatenate([g, tail], axis=1)
        parts = [halves(joined)]
        if not line:
            whole = lax.all_gather(g, "horizon", axis=0)
            if c == 0:
                all_discount = wide(whole[:, 0, lanes:lanes + width]) + wide(whole[:, 1, lanes:lanes + width]) / FINE
                lower_by = jnp.exp2(-wide(whole[:, :, lanes + width:lanes + width + 1]))
            high, low = halves((wide(whole[:, :, :lanes]) * lower_by).reshape(n_hor * cols, lanes))
            part = product([high, low], [expect], scales, 0, [at], n, assets)
            pieces = part if pieces is None else pieces + part
            at += n
            continue
        last = c == len(counts) - 1
        with scope(f"swap{c}"):
            a = lax.ppermute(g, "horizon", inward if last else inward + outward)
        with scope(f"cross{c}"):
            b1 = lax.ppermute(g, "horizon", middle)
        with scope(f"crossnext{c}"):
            b2 = lax.ppermute(a, "horizon", middle)
        if last:
            got = [wide(a), wide(b1), wide(b2)]
        else:
            with scope(f"out{c}"):
                c1 = lax.ppermute(b1, "horizon", outward)
            with scope(f"outnext{c}"):
                c2 = lax.ppermute(b2, "horizon", outward)
            got = [wide(a), wide(b1) + wide(c1), wide(b2) + wide(c2)]
        if c == 0:
            lit = jnp.stack([wide(tail[:2, :width])] + [v[:2, lanes:lanes + width] for v in got])
            all_discount = lit[:, 0] + lit[:, 1] / FINE
            lower_by = [jnp.exp2(-v[:, lanes + width:lanes + width + 1]) for v in got]
        parts += [halves(v[:, :lanes] * by) for v, by in zip(got, lower_by)]
        lefts = [p[0] for p in parts] + [p[1] for p in parts]
        if not last:
            with scope(f"product{c}"):
                part = product(lefts, [expect], scales, 0, [at], n, assets)
            pieces = part if pieces is None else pieces + part
            at += n
            continue
        left_at = 0
        for i, (m, rows) in enumerate(zip(helped, moved)):
            with scope(f"helped{i}"):
                part = product(lefts, [expect, rows], scales, left_at, [at + left_at, 0], m, assets)
            pieces = pieces + part[:, :width]
            aside = part[:, width:] if aside is None else aside + part[:, width:]
            left_at += m
    if line:
        order = jnp.array([[0, 1, 2, 3], [1, 0, 2, 3], [3, 2, 0, 1], [3, 2, 1, 0]], jnp.int32)[me]
        place = lambda v: jnp.take(v.reshape(n_hor, -1, v.shape[-1]), order, axis=0)
        flow = place(pieces).reshape(n_hor * cols, width)
        flow_help = place(aside.reshape(n_hor, cols, width).at[1].set(0.0)).reshape(n_hor * cols, width)
        all_discount = place(all_discount[:, None, :])[:, 0]
    else:
        flow, flow_help = pieces, jnp.zeros_like(pieces)

    left_help = jnp.where(me < n_hor // 2, flow_help, 0.0)
    spread = jnp.concatenate([left_help, flow, flow_help - left_help], axis=1)
    spread = diagonal(spread)
    share = spread.shape[0] // n_state
    spread = lax.all_to_all(spread.reshape(n_state, share, 3 * width), "state", 0, 0)
    spread = jnp.sum(spread, axis=0)

    log_rates = jnp.log(all_discount)
    before = jnp.cumsum(log_rates, axis=1) - log_rates
    totals = jnp.sum(log_rates, axis=1)
    reach = jnp.concatenate([jnp.zeros((1,)), jnp.cumsum(totals)])
    inside = jnp.pad(jnp.exp(before), ((1, 1), (0, 0)))
    mine = lax.dynamic_slice_in_dim(inside, me, 3, 0)
    ahead = jnp.einsum("sbw,bw->bs", spread.reshape(share, 3, width), mine, precision=lax.Precision.HIGHEST)
    ids = jnp.arange(n_hor)
    source = me - 1 + jnp.arange(3)
    gap = jnp.where((source[None, :] > ids[:, None]) & (source[None, :] < n_hor) & (source[None, :] >= 0),
                    jnp.exp(reach[jnp.clip(source, 0, n_hor)][None, :] - reach[1:][:, None]), 0.0)
    later = jnp.einsum("hb,bs->hs", gap, ahead, precision=lax.Precision.HIGHEST)
    place = (source[None, :] == ids[:, None]).astype(jnp.float32)
    own_part = jnp.einsum("hb,sbw->hsw", place, spread.reshape(share, 3, width), precision=lax.Precision.HIGHEST)
    message = jnp.concatenate([own_part, jnp.broadcast_to(later[:, :, None], (n_hor, share, LANES))], axis=2)
    message = jnp.sum(lax.all_to_all(message, "horizon", 0, 0), axis=0)
    jac = message[:, :width]
    incoming = message[:, width:width + 1]

    log_own = jnp.log(discount)
    before_own = jnp.cumsum(log_own) - log_own
    rows = lax.broadcasted_iota(jnp.int32, (width, width), 0)
    columns = lax.broadcasted_iota(jnp.int32, (width, width), 1)
    ladder = jnp.where(rows >= columns, jnp.exp(jnp.minimum(before_own[:, None] - before_own[None, :], 0.0)), 0.0)
    value = jnp.dot(jac, ladder, precision=lax.Precision.HIGHEST)
    value = value + incoming * jnp.exp(jnp.sum(log_own) - before_own)[None, :]
    return jac, value


def solution(mesh):
    return jax.shard_map(
        local,
        mesh=mesh,
        in_specs=(
            P("horizon", "state"),
            P("state"),
            P("horizon", "state"),
            P("state", None),
            P(),
            P("state", None, None),
            P("horizon"),
        ),
        out_specs=(P("state", "horizon"), P("state", "horizon")),
        check_vma=False,
    )
```

```python
import functools

import jax
import jax.numpy as jnp
from jax import lax
from jax.experimental import pallas as pl
from jax.experimental.pallas import tpu as pltpu
from jax.sharding import PartitionSpec as P


LANES = 128
GROUP = 16
VMEM_LIMIT = 67_000_000


def type_chunks(types):
    helped = [max(types // 16, 1), types // 4]
    plain = [max(types // 8, 1), types // 4]
    return plain + [types - sum(plain) - sum(helped)], helped


def shift_kernel(types, blocks, counts, starts, policy, steady, index, trans, rates, *refs):
    outs, (landed, rows, sems) = refs[:-3], refs[-3:]
    assets = blocks * LANES
    cols = policy.shape[0]
    groups = cols // GROUP
    fetch = lambda x: pltpu.make_async_copy(
        policy.at[:, pl.ds(pl.multiple_of(x * assets, LANES), assets)], rows.at[x], sems.at[x])
    for x in range(types):
        fetch(x).start()
    targets = lax.broadcasted_iota(jnp.int32, (2 * LANES, LANES), 0).astype(jnp.float32).astype(jnp.bfloat16)
    one = jnp.ones((2 * LANES, LANES), jnp.bfloat16)
    zero = jnp.zeros((2 * LANES, LANES), jnp.bfloat16)

    def land(x, carry):
        fetch(x).wait()
        landed[:, x] = jnp.zeros(landed.shape[:1] + landed.shape[2:], jnp.float32)
        offsets, weights = index[x], steady[x]
        for k in range(blocks):
            cut = slice(k * LANES, (k + 1) * LANES)
            begin = starts[x, k] * LANES
            offset = (offsets[k:k + 1, :] - begin).astype(jnp.float32)
            low = offset.astype(jnp.bfloat16)
            high = (offset + 1.0).astype(jnp.bfloat16)
            lottery = jnp.where(targets == low, one, jnp.where(targets == high, -one, zero))
            mass = (weights[k:k + 1, :] * rows[x, :, cut].astype(jnp.float32)).astype(jnp.bfloat16)
            moved = lax.dot_general(mass, lottery, (((1,), (1,)), ((), ())), preferred_element_type=jnp.float32)
            window = pl.ds(pl.multiple_of(begin, LANES), 2 * LANES)
            for g in range(groups):
                landed[g, x, :, window] += moved[g * GROUP:(g + 1) * GROUP]
        return carry

    lax.fori_loop(0, types, land, 0)

    dot = functools.partial(jnp.dot, preferred_element_type=jnp.float32)
    size = types * GROUP
    row = lax.broadcasted_iota(jnp.int32, (size, size), 0) % GROUP
    col = lax.broadcasted_iota(jnp.int32, (size, size), 1) % GROUP
    mix = trans[...] / jnp.sum(trans[...], axis=1, keepdims=True)
    mix_first = mix.astype(jnp.bfloat16)
    mix_second = (mix - mix_first.astype(jnp.float32)).astype(jnp.bfloat16)
    pick = (lax.broadcasted_iota(jnp.int32, (types, size), 1) // GROUP
            == lax.broadcasted_iota(jnp.int32, (types, size), 0)).astype(jnp.float32).astype(jnp.bfloat16)

    def spread(part):
        rows = lax.dot_general(part, pick, (((0,), (0,)), ((), ())), preferred_element_type=jnp.float32)
        rows = jnp.concatenate(
            [jnp.broadcast_to(rows[y:y + 1, :], (GROUP, size)) for y in range(types)], axis=0)
        return jnp.where(row == col, rows, 0.0).astype(jnp.bfloat16)

    mix_hi, mix_lo = spread(mix_first), spread(mix_second)
    wide = 2 * LANES

    def tile(j, peaks):
        lanes = pl.ds(pl.multiple_of(j * wide, wide), wide)
        peaks = list(peaks)
        for g in range(groups):
            value = landed[g, :, :, lanes].reshape(size, wide)
            hi = value.astype(jnp.bfloat16)
            lo = (value - hi.astype(jnp.float32)).astype(jnp.bfloat16)
            blended = dot(mix_hi, hi) + dot(mix_hi, lo) + dot(mix_lo, hi)
            y = 0
            for c, count in enumerate(counts):
                for i in range(count):
                    outs[c][g * GROUP:(g + 1) * GROUP,
                            pl.ds(pl.multiple_of(i * assets + j * wide, wide), wide)] = (
                        blended[y * GROUP:(y + 1) * GROUP].astype(jnp.bfloat16))
                    peaks[g] = jnp.maximum(peaks[g], jnp.abs(blended[y * GROUP:(y + 1) * GROUP]))
                    y += 1
        return tuple(peaks)

    peaks = lax.fori_loop(0, assets // wide, tile, (jnp.zeros((GROUP, wide), jnp.float32),) * groups)
    peak = jnp.concatenate([jnp.max(p, axis=1, keepdims=True) for p in peaks], axis=0)
    lane = lax.broadcasted_iota(jnp.int32, (cols, LANES), 1)
    down = (lax.broadcasted_iota(jnp.int32, (cols, 2), 0)
            == lax.broadcasted_iota(jnp.int32, (cols, 2), 1)).astype(jnp.float32).astype(jnp.bfloat16)
    across = (lax.broadcasted_iota(jnp.int32, (types, LANES), 0)
              == lax.broadcasted_iota(jnp.int32, (types, LANES), 1)).astype(jnp.float32).astype(jnp.bfloat16)
    placed = dot(dot(down, rates[0]).astype(jnp.bfloat16), across)
    outs[0][:, counts[0] * assets:] = jnp.where(lane < LANES // 2, placed, peak).astype(jnp.bfloat16)


def build_shift(policy, steady, index, type_trans, migration, counts):
    cols = policy.shape[0]
    types, assets = index.shape
    blocks = assets // LANES
    index = index.reshape(types, blocks, LANES)
    starts = jnp.min(index, axis=2) >> (LANES.bit_length() - 1)
    shapes = [jax.ShapeDtypeStruct((cols, n * assets + (0 if c else LANES)), jnp.bfloat16)
              for c, n in enumerate(counts)]
    whole = lambda shape: pl.BlockSpec(shape, lambda x, *_: (0,) * len(shape))
    return pl.pallas_call(
        functools.partial(shift_kernel, types, blocks, tuple(counts)),
        out_shape=shapes,
        grid_spec=pltpu.PrefetchScalarGridSpec(
            num_scalar_prefetch=1,
            grid=(1,),
            in_specs=[
                pl.BlockSpec(memory_space=pl.ANY),
                whole((types, blocks, LANES)),
                whole((types, blocks, LANES)),
                whole(type_trans.shape),
                whole(migration.shape),
            ],
            out_specs=[whole(s.shape) for s in shapes],
            scratch_shapes=[
                pltpu.VMEM((cols // GROUP, types, GROUP, assets + LANES), jnp.float32),
                pltpu.VMEM((types, cols, assets), jnp.bfloat16),
                pltpu.SemaphoreType.DMA((types,)),
            ],
        ),
        compiler_params=pltpu.CompilerParams(
            dimension_semantics=("arbitrary",), vmem_limit_bytes=VMEM_LIMIT),
        cost_estimate=pl.CostEstimate(flops=10**10, bytes_accessed=2**23, transcendentals=0),
        name="build_shift",
    )(starts, policy, steady.reshape(types, blocks, LANES), index, type_trans, migration)


def mix_kernel(count, assets, types, at, *refs):
    own, above, below, own_note, above_note, below_note = refs[:6]
    tail = refs[6] if len(refs) == 8 else None
    out = refs[-1]
    lane = lax.broadcasted_iota(jnp.int32, (1, LANES), 1)
    note = lambda ref: ref[...].astype(jnp.float32)
    own_row, above_row, below_row = note(own_note), note(above_note), note(below_note)
    stay = 1.0 - own_row[0:1] - own_row[1:2]
    down, up = above_row[0:1], below_row[1:2]
    top = lambda rate: jnp.max(jnp.where(lane < types, rate, 0.0), axis=1, keepdims=True)
    half = LANES // 2
    peak = lambda rows: rows[:, half:half + 1]
    bound = top(stay) * peak(own_row) + top(down) * peak(above_row) + top(up) * peak(below_row)
    power = jnp.clip(14.9 - jnp.log2(jnp.maximum(bound, 1e-30)), -100.0, 100.0)
    power = jnp.floor(power)
    scale = jnp.exp2(power)
    for i in range(count):
        one = lambda rate: jnp.sum(jnp.where(lane == at + i, rate, 0.0), axis=1, keepdims=True)
        span = slice(i * assets, (i + 1) * assets)
        value = ((own[:, span].astype(jnp.float32) * one(stay)
                  + above[:, span].astype(jnp.float32) * one(down))
                 + below[:, span].astype(jnp.float32) * one(up))
        out[:, span] = jnp.round(value * scale).astype(jnp.int32).astype(jnp.int16)
    if tail is not None:
        edge = count * assets
        width = tail.shape[1]
        out[:, edge:edge + width] = tail[...]
        out[:, edge + width:] = jnp.broadcast_to(power, (power.shape[0], LANES)).astype(jnp.int32).astype(jnp.int16)


def mix(own, above, below, notes, edge, tail, at, count, assets, types):
    cols = own.shape[0]
    extra = 0 if tail is None else tail.shape[1] + LANES
    body = pl.BlockSpec((cols, count * assets), lambda i: (0, 0))
    note = pl.BlockSpec((cols, LANES), lambda i: (0, edge // LANES))
    tails = [] if tail is None else [tail]
    return pl.pallas_call(
        functools.partial(mix_kernel, count, assets, types, at),
        out_shape=jax.ShapeDtypeStruct((cols, count * assets + extra), jnp.int16),
        grid=(1,),
        in_specs=[body] * 3 + [note] * 3 + [pl.BlockSpec(t.shape, lambda i: (0, 0)) for t in tails],
        out_specs=pl.BlockSpec((cols, count * assets + extra), lambda i: (0, 0)),
        compiler_params=pltpu.CompilerParams(
            dimension_semantics=("arbitrary",), vmem_limit_bytes=VMEM_LIMIT),
        cost_estimate=pl.CostEstimate(
            flops=2**12 * cols * count * assets, bytes_accessed=8 * cols * count * assets, transcendentals=0),
        name="mix",
    )(own, above, below, *notes, *tails)


def finish(total, base, lower, order, out, parts):
    blocks = lower.shape[0] // parts
    width = base.shape[1]
    total[:, :width] = (total[:, :width] + base[...]) * lower[...]
    total[:, width:] = total[:, width:] * lower[...]
    total[blocks:2 * blocks, width:] = jnp.zeros((blocks, width), jnp.float32)
    left = order[parts].astype(jnp.float32)
    rows = []
    for b in range(parts):
        block = total[pl.ds(pl.multiple_of(order[b] * blocks, 8), blocks), :]
        aside = block[:, width:]
        rows.append(jnp.concatenate([aside * left, block[:, :width], aside * (1.0 - left)], axis=1))
    value = jnp.concatenate(rows, axis=0)
    row = lax.broadcasted_iota(jnp.int32, value.shape, 0)
    lane = lax.broadcasted_iota(jnp.int32, value.shape, 1)
    offset = 1
    while offset < value.shape[0]:
        moved = pltpu.roll(pltpu.roll(value, offset, 0), offset, 1)
        value = value + jnp.where((row >= offset) & (lane >= offset), moved, 0.0)
        offset *= 2
    out[...] = value


def product_kernel(segments, n_in, assets, width, parts, stay, *refs):
    if parts:
        order, refs = refs[0], refs[1:]
        sources, (base, lower, result, out), buffers, sems = refs[:n_in], (
            refs[n_in], refs[n_in + 1], refs[n_in + 2], refs[-2]), refs[n_in + 3:-2], refs[-1]
    else:
        sources, out, buffers, sems = refs[:n_in], refs[n_in], refs[n_in + 1:-1], refs[-1]

    def fetch(slot, i, j, at):
        at = pl.multiple_of((at + i) * assets, LANES)
        return pltpu.make_async_copy(sources[j].at[:, pl.ds(at, assets)], buffers[slot].at[i], sems.at[slot, i])

    slot = 0
    plans = []
    for groups, rights, count in segments:
        slots = []
        for j, at in [item for group in groups for item in group] + rights:
            slots.append((slot, j, at))
            slot += 1
        plans.append(slots)
        for i in range(count):
            for s, j, at in slots:
                fetch(s, i, j, at).start()
    out[...] = jnp.zeros_like(out)

    for (groups, rights, count), slots in zip(segments, plans):
        first = rights[0][1]

        def one(i, carry):
            for s, j, at in slots:
                fetch(s, i, j, at).wait()
            scale = stay[0, first + i]
            undo = stay[1, first + i]
            highs, lows = [], []
            s = slots[0][0]
            for group in groups:
                units = sum(b[i].astype(jnp.int32) for b in buffers[s:s + len(group)])
                s += len(group)
                value = units.astype(jnp.float32)
                high = value.astype(jnp.bfloat16)
                highs.append(high)
                lows.append((value - high.astype(jnp.float32)).astype(jnp.bfloat16))
            left = jnp.concatenate(highs + lows, axis=0)
            sides = []
            for r in range(len(rights)):
                exact = buffers[s + r][i]
                value = exact.astype(jnp.float32)
                home = (value * scale).astype(jnp.bfloat16).astype(jnp.float32)
                sides += [exact, (home * undo - value).astype(jnp.bfloat16)]
            right = jnp.concatenate(sides, axis=0)
            total = lax.dot_general(left, right, (((1,), (1,)), ((), ())), preferred_element_type=jnp.float32)
            half = total.shape[0] // 2
            both = total[:half] + total[half:]
            for r in range(len(rights)):
                base = 2 * r * width
                out[:, r * width:(r + 1) * width] += (
                    both[:, base:base + width] + both[:, base + width:base + 2 * width])
            return carry

        lax.fori_loop(0, count, one, 0)
    if parts:
        finish(out, base, lower, order, result, parts)


def product(jobs, stay, assets, base=None, lower=None, order=None):
    inputs, segments, buffers = [], [], []

    def slot(item, count):
        value, at = item
        for j, known in enumerate(inputs):
            if known is value:
                break
        else:
            j = len(inputs)
            inputs.append(value)
        buffers.append(pltpu.VMEM((count, value.shape[0], assets), value.dtype))
        return j, at

    for groups, rights, count in jobs:
        segments.append(([[slot(item, count) for item in group] for group in groups],
                         [slot(item, count) for item in rights], count))
    rows = sum(group[0][0].shape[0] for group in jobs[0][0])
    width = jobs[0][1][0][0].shape[0]
    cols = width * max(len(rights) for _, rights, _ in jobs)
    total = sum(count for _, _, count in jobs)
    end = base is not None
    whole = lambda v: pl.BlockSpec(v.shape, lambda i, *_: (0, 0))
    result = jax.ShapeDtypeStruct((rows, 3 * width if end else cols), jnp.float32)
    return pl.pallas_call(
        functools.partial(product_kernel, segments, len(inputs), assets, width, order.shape[0] - 1 if end else 0),
        out_shape=result,
        grid_spec=pltpu.PrefetchScalarGridSpec(
            num_scalar_prefetch=2 if end else 1,
            grid=(1,),
            in_specs=[pl.BlockSpec(memory_space=pl.ANY)] * len(inputs) + ([whole(base), whole(lower)] if end else []),
            out_specs=whole(result),
            scratch_shapes=buffers + ([pltpu.VMEM((rows, cols), jnp.float32)] if end else []) + [
                pltpu.SemaphoreType.DMA((len(buffers), max(count for _, _, count in jobs)))],
        ),
        compiler_params=pltpu.CompilerParams(
            dimension_semantics=("arbitrary",), vmem_limit_bytes=VMEM_LIMIT),
        cost_estimate=pl.CostEstimate(
            flops=8 * rows * cols * total * assets, bytes_accessed=2 * (rows + cols) * total * assets,
            transcendentals=0),
        name="product",
    )(stay, *([order] if end else []), *inputs, *([base, lower] if end else []))


def wide(value):
    return value.astype(jnp.float32)


def diagonal(block):
    rows, width = block.shape
    offset = 1
    while offset < rows:
        block = block + jnp.pad(block, ((offset, 0), (offset, 0)))[:rows, :width]
        offset *= 2
    return block


FINE = 4096.0


def step(expect, steady_dist, policy_deriv, lottery_index, type_trans, migration, discount):
    types, assets = lottery_index.shape
    n_state, n_hor = lax.axis_size("state"), lax.axis_size("horizon")
    width = expect.shape[0]
    cols = policy_deriv.shape[0]
    line = n_hor == 4
    plain, helped = type_chunks(types)
    if not line:
        plain, helped = plain + helped, []
    counts = plain + ([sum(helped)] if helped else [])

    coarse = jnp.floor(discount * FINE)
    fine = jnp.round((discount * FINE - coarse) * FINE)
    tail = jnp.pad(jnp.stack([coarse, fine]), ((0, cols - 2), (0, 0))).astype(jnp.int16)

    up = [(i, (i + 1) % n_state) for i in range(n_state)]
    down = [((i + 1) % n_state, i) for i in range(n_state)]
    inward = [(0, 1), (n_hor - 1, n_hor - 2)]
    outward = [(1, 0), (n_hor - 2, n_hor - 1)]
    middle = [(1, 2), (2, 1)]
    moved = []

    def lend(rows, i):
        first = (sum(plain) + sum(helped[:i])) * assets
        moved.append(lax.ppermute(rows[:, first:first + helped[i] * assets], "horizon", inward))

    if line:
        lend(expect, 0)

    shift = build_shift(policy_deriv, steady_dist, lottery_index, type_trans, migration, counts)
    above, below = [], []
    for d in shift:
        above.append(lax.ppermute(d, "state", down))
        below.append(lax.ppermute(d, "state", up))

    notes = [shift[0], above[0], below[0]]
    edge = counts[0] * assets
    jobs = []
    at = 0
    for c, n in enumerate(counts):
        g = mix(shift[c], above[c], below[c], notes, edge, None if c else tail, at, n, assets, types)
        if c == 1:
            late_rates, late_discount, me, _ = lax.optimization_barrier(
                (migration, discount, lax.axis_index("horizon"), g))
            own = wide(late_rates[0])
            stay = 1.0 - own[0] - own[1]
            scales = jnp.stack([stay, 1.0 / stay])
        if c == len(plain) - 1 and line:
            late_expect, _ = lax.optimization_barrier((expect, g))
            for i in range(1, len(helped)):
                lend(late_expect, i)
        if not line:
            whole = lax.all_gather(g, "horizon", axis=0)
            got = [[whole[h]] for h in range(n_hor)]
        else:
            last = c == len(counts) - 1
            a = lax.ppermute(g, "horizon", inward if last else inward + outward)
            b1 = lax.ppermute(g, "horizon", middle)
            b2 = lax.ppermute(a, "horizon", middle)
            got = [[g], [a], [b1], [b2]]
            if not last:
                got[2].append(lax.ppermute(b1, "horizon", outward))
                got[3].append(lax.ppermute(b2, "horizon", outward))
        jobs.append((got, n, at))
        at += n

    job = lambda rows, rights, left_at, n: ([[(v, left_at) for v in group] for group in rows], rights, n)
    plain_jobs = [job(rows, [(expect, first)], 0, n) for rows, n, first in jobs[:len(plain)]]
    first_rows, _ = lax.optimization_barrier((jobs[0][0], jobs[-1][0][0]))
    lit = jnp.stack([wide(sum(v[:, edge:] for v in group)) for group in first_rows])
    all_discount = (lit[:, 0, :width] + lit[:, 1, :width] / FINE) / FINE
    lower_by = jnp.exp2(-lit[:, :, width]).reshape(n_hor * cols, 1)
    if line:
        pieces = product(plain_jobs[:-1], scales, assets)
        rows, _, first = jobs[-1]
        last_jobs, left_at = plain_jobs[-1:], 0
        for n, rights in zip(helped, moved):
            last_jobs.append(job(rows, [(expect, first + left_at), (rights, 0)], left_at, n))
            left_at += n
        order = jnp.array([[0, 1, 2, 3, 1], [1, 0, 2, 3, 1], [3, 2, 0, 1, 0], [3, 2, 1, 0, 0]], jnp.int32)[me]
        spread = product(last_jobs, scales, assets, pieces, lower_by, order)
        all_discount = jnp.take(all_discount, order[:n_hor], axis=0)
    else:
        flow = product(plain_jobs, scales, assets) * lower_by
        blank = jnp.zeros_like(flow)
        spread = diagonal(jnp.concatenate([blank, flow, blank], axis=1))
    share = spread.shape[0] // n_state
    spread = lax.all_to_all(spread.reshape(n_state, share, 3 * width), "state", 0, 0)
    spread = jnp.sum(spread, axis=0)

    log_rates = jnp.log(all_discount)
    before = jnp.cumsum(log_rates, axis=1) - log_rates
    totals = jnp.sum(log_rates, axis=1)
    reach = jnp.concatenate([jnp.zeros((1,)), jnp.cumsum(totals)])
    inside = jnp.pad(jnp.exp(before), ((1, 1), (0, 0)))
    mine = lax.dynamic_slice_in_dim(inside, me, 3, 0)
    ahead = jnp.einsum("sbw,bw->bs", spread.reshape(share, 3, width), mine, precision=lax.Precision.HIGHEST)
    ids = jnp.arange(n_hor)
    source = me - 1 + jnp.arange(3)
    gap = jnp.where((source[None, :] > ids[:, None]) & (source[None, :] < n_hor) & (source[None, :] >= 0),
                    jnp.exp(reach[jnp.clip(source, 0, n_hor)][None, :] - reach[1:][:, None]), 0.0)
    later = jnp.einsum("hb,bs->hs", gap, ahead, precision=lax.Precision.HIGHEST)
    place = (source[None, :] == ids[:, None]).astype(jnp.float32)
    own_part = jnp.einsum("hb,sbw->hsw", place, spread.reshape(share, 3, width), precision=lax.Precision.HIGHEST)
    message = jnp.concatenate([own_part, jnp.broadcast_to(later[:, :, None], (n_hor, share, LANES))], axis=2)
    message = jnp.sum(lax.all_to_all(message, "horizon", 0, 0), axis=0)
    jac = message[:, :width]
    incoming = message[:, width:width + 1]

    log_own = jnp.log(late_discount)
    before_own = jnp.cumsum(log_own) - log_own
    rows = lax.broadcasted_iota(jnp.int32, (width, width), 0)
    columns = lax.broadcasted_iota(jnp.int32, (width, width), 1)
    ladder = jnp.where(rows >= columns, jnp.exp(jnp.minimum(before_own[:, None] - before_own[None, :], 0.0)), 0.0)
    value = jnp.dot(jac, ladder, precision=lax.Precision.HIGHEST)
    value = value + incoming * jnp.exp(jnp.sum(log_own) - before_own)[None, :]
    return jac, value


def solution(mesh):
    return jax.shard_map(
        step,
        mesh=mesh,
        in_specs=(
            P("horizon", "state"),
            P("state"),
            P("horizon", "state"),
            P("state", None),
            P(),
            P("state", None, None),
            P("horizon"),
        ),
        out_specs=(P("state", "horizon"), P("state", "horizon")),
        check_vma=False,
    )
```
